32 devices in a mesh: groups: 2 (over y), blk: 4 (over z), ulysses: 2 (over x), cfg: 2 (over core).
Axes of the slice: x: 2, y: 2, z: 4, core: 2. Of those that a mesh axis runs over, the one named last changes fastest.
Arguments:
- img_tokens: bfloat16 [2, 2, 512, 2432], P('cfg', 'groups', ('blk', 'ulysses')), parts along dimension 1, may hold values from -72 to 72
- text_tokens: bfloat16 [2, 2, 48, 2432], P('cfg', 'groups', ('blk', 'ulysses')), parts along dimension 1, may hold values from -6 to 6
- text_lengths: int32 [2, 2], P('cfg', 'groups'), parts along dimension 1, may hold values from 12 to 48
- timestep: int32 [2], P('groups'), parts along dimension 0, may hold values from 0 to 999
- pooled: float32 [2, 2, 2432], P(None, 'groups'), parts along dimension 1, may hold values from -6 to 6
- time_weight: bfloat16 [256, 2432], replicated, may hold values from -0.375 to 0.375
- time_second: bfloat16 [2432, 2432], P(None, ('blk', 'ulysses', 'cfg')), may hold values from -0.125 to 0.125
- mod_weight: bfloat16 [2432, 24320], P(None, ('blk', 'ulysses', 'cfg')), may hold values from -0.125 to 0.125
- proj_weight: bfloat16 [5, 2432, 2048], P(None, None, ('ulysses', 'cfg')), may hold values from -0.125 to 0.125
- out_weight: bfloat16 [2048, 2432], P(('ulysses', 'cfg')), may hold values from -0.125 to 0.125
- expand_weight: bfloat16 [2432, 7168], P('blk', ('ulysses', 'cfg')), may hold values from -0.125 to 0.125
- reduce_weight: bfloat16 [7168, 2432], P(('ulysses', 'cfg'), 'blk'), may hold values from -0.0625 to 0.0625
- qk_gain: float32 [3, 64], replicated, may hold values from 0.5 to 10
- final_weight: bfloat16 [2432, 64], replicated, may hold values from -0.125 to 0.125
Outputs:
- guided: float32 [2, 16, 16, 128], P('groups', None, ('blk', 'ulysses', 'cfg')), parts along dimension 0
The draws below stay inside these ranges and needn't reach their ends.
There are 2 independent parts, one for each index of `groups`. The reference program is written for one: setup_inputs(seed, part) draws one part's arguments, and reference() takes and returns one part's arrays. A program takes and returns all parts, laid end to end along the dimension named above; an argument that names none is the same for every part. Nothing has to cross between parts.
All inputs are finite; a program needn't handle non-finite values.
Results may differ from the reference program's by a relative error of at most 0.011.
The reference program's roundings to bfloat16 on the way count: a program that leaves them out, or rounds other values in their place, can miss the bound.
Values may be sent and summed in bfloat16 or wider, within the bound.
No kernel may reach another device: no remote copies, remote signals or barrier semaphores. Data moves between devices by JAX's collectives and lax.ppermute only.
A program may use at most 192 MiB of HBM per device.

```python
import math
import jax
import jax.numpy as jnp
from jax import lax

D = 2432
HEADS = 32
HD = 64
LAT = 16
FREQ = 256
FF = 7168
PROMPTS = 1
IMG_DEV = 64
INNER = 2048
PATCH_OUT = 64
IMG = 512
TXT = 48
N_ULYSSES = 2
N_CFG = 2


def draw_img_tokens(key, part):
    base_key, row_key, col_key = jax.random.split(jax.random.fold_in(key, 11), 3)
    full_shape = (2, PROMPTS, IMG, D)
    base_draw = jnp.clip(jax.random.normal(base_key, full_shape, jnp.float32), -4.0, 4.0)
    row_top = math.log(4.0)
    row_scale = jnp.exp(jax.random.uniform(row_key, (2, PROMPTS, IMG, 1), jnp.float32, 0.0, row_top))
    col_scale = jnp.exp(jax.random.uniform(col_key, (1, 1, 1, D), jnp.float32, math.log(0.5), math.log(2.0)))
    return (base_draw * row_scale * col_scale).astype(jnp.bfloat16)


def draw_qk_gain(key, part):
    gain_key = jax.random.fold_in(key, 23)
    low_end = math.log(0.5)
    high_end = math.log(2.0)
    return jnp.exp(jax.random.uniform(gain_key, (3, HD), jnp.float32, low_end, high_end))


def shard_levels(key, shape, cuts, smallest, largest):
    def one(position, blocks):
        heights = jax.random.uniform(jax.random.fold_in(jax.random.fold_in(key, 6), position), (blocks,), jnp.float32, smallest / len(cuts), largest / len(cuts))
        return jnp.repeat(jnp.exp(heights), shape[position] // blocks).reshape((-1,) + (1,) * (len(shape) - position - 1))

    level = one(*cuts[0])
    for cut in cuts[1:]:
        level = level * one(*cut)
    return level


def normal_values(stream_key, dims, deviation, bound, shards=(), kind=jnp.bfloat16):
    factor_of = shard_levels(stream_key, dims, shards, -0.22, 0.18) if shards else 1.0
    result = jax.random.normal(stream_key, dims, jnp.float32) * deviation * factor_of
    return jnp.minimum(jnp.maximum(result, -bound), bound).astype(kind)


def setup_inputs(seed: int = 0, part: int = 0) -> dict:
    key_list = jax.random.split(jax.random.key(seed), 15)
    part_keys = jax.random.split(jax.random.fold_in(key_list[14], part), 15)
    img_tokens = draw_img_tokens(jax.random.fold_in(jax.random.fold_in(key_list[14], part), 71), part)
    text_tokens = normal_values(part_keys[1], (2, PROMPTS, TXT, D), 1.0, 6.0, ((0, 2), (2, 8)))
    text_lengths = jax.random.randint(part_keys[2], (2, PROMPTS), TXT // 4, TXT + 1).astype(jnp.int32)
    timestep = jax.random.randint(part_keys[3], (PROMPTS,), 0, 1000).astype(jnp.int32)
    pooled = normal_values(part_keys[4], (2, PROMPTS, D), 1.0, 6.0, (), jnp.float32)
    time_weight = normal_values(key_list[5], (FREQ, D), FREQ ** -0.5, 0.375)
    time_second = normal_values(key_list[6], (D, D), D ** -0.5, 0.125, ((1, 16),))
    mod_weight = normal_values(key_list[7], (D, 10 * D), D ** -0.5, 0.125, ((1, 16),))
    proj_weight = normal_values(key_list[8], (5, D, INNER), D ** -0.5, 0.125, ((2, 4),))
    out_weight = normal_values(key_list[9], (INNER, D), INNER ** -0.5, 0.125, ((0, 4),))
    expand_weight = normal_values(key_list[10], (D, FF), D ** -0.5, 0.125, ((0, 4), (1, 4)))
    reduce_weight = normal_values(key_list[11], (FF, D), FF ** -0.5, 0.0625, ((0, 4), (1, 4)))
    qk_gain = draw_qk_gain(jax.random.fold_in(key_list[14], 71), part)
    final_weight = normal_values(key_list[13], (D, PATCH_OUT), D ** -0.5, 0.125)
    return {"img_tokens": img_tokens, "text_tokens": text_tokens, "text_lengths": text_lengths, "timestep": timestep, "pooled": pooled, "time_weight": time_weight, "time_second": time_second, "mod_weight": mod_weight, "proj_weight": proj_weight, "out_weight": out_weight, "expand_weight": expand_weight, "reduce_weight": reduce_weight, "qk_gain": qk_gain, "final_weight": final_weight}


GUIDANCE = 3.5
LN_EPS = 1e-06
RMS_EPS = 1e-06
NEG_FILL = -1e+30

def sinusoid(timestep, feature_count):
    half_width = feature_count // 2
    frequency = jnp.exp(-math.log(10000.0) * jnp.arange(half_width, dtype=jnp.float32) / half_width)
    angles = timestep.astype(jnp.float32)[:, None] * frequency[None, :]
    return jnp.concatenate([jnp.cos(angles), jnp.sin(angles)], axis=1)

def layer_norm(values):
    average = lax.optimization_barrier(jnp.mean(values, axis=-1, keepdims=True))
    centred = values - average
    variance = lax.optimization_barrier(jnp.mean(centred * centred, axis=-1, keepdims=True))
    return centred * lax.rsqrt(variance + LN_EPS)

def modulate(values, shift, scale):
    return (layer_norm(values.astype(jnp.float32)) * (1.0 + scale) + shift).astype(jnp.bfloat16)

def rms_heads(values, gain):
    head_size = gain.shape[0]
    shaped = values.reshape(values.shape[:-1] + (values.shape[-1] // head_size, head_size))
    inverse = lax.rsqrt(lax.optimization_barrier(jnp.mean(shaped * shaped, axis=-1, keepdims=True)) + RMS_EPS)
    return (shaped * inverse * gain).reshape(values.shape).astype(jnp.bfloat16)

def finish(img_proj, txt_proj, gain_rows):
    img_set = jnp.stack([rms_heads(img_proj[0], gain_rows[0]), rms_heads(img_proj[1], gain_rows[1]), img_proj[2].astype(jnp.bfloat16)])
    txt_set = jnp.stack([rms_heads(txt_proj[0], gain_rows[2]), txt_proj[1].astype(jnp.bfloat16)])
    return (img_set, txt_set)

def head_attention(query_head, key_head, value_head, usable):
    scores = jnp.dot(query_head, key_head.T, preferred_element_type=jnp.float32) * (1.0 / math.sqrt(query_head.shape[1]))
    scores = jnp.where(usable[None, :], scores, NEG_FILL)
    row_max = lax.optimization_barrier(jnp.max(scores, axis=1, keepdims=True))
    weights = jnp.where(usable[None, :], jnp.exp(scores - row_max), 0.0)
    row_total = lax.optimization_barrier(jnp.sum(weights, axis=1, keepdims=True))
    mixed = jnp.dot(weights.astype(jnp.bfloat16), value_head, preferred_element_type=jnp.float32) / row_total
    return mixed.astype(jnp.bfloat16)

def feed_forward(feed_input, expand_weight, reduce_weight):
    feed_hidden = jax.nn.gelu(jnp.dot(feed_input, expand_weight, preferred_element_type=jnp.float32), approximate=True).astype(jnp.bfloat16)
    group_count = N_ULYSSES * N_CFG
    group_width = reduce_weight.shape[0] // group_count
    feed_out = jnp.zeros((feed_input.shape[0], reduce_weight.shape[1]), jnp.float32)
    for group in range(group_count):
        term = jnp.dot(feed_hidden[:, group * group_width:(group + 1) * group_width], reduce_weight[group * group_width:(group + 1) * group_width], preferred_element_type=jnp.float32)
        term = lax.optimization_barrier(term.astype(jnp.bfloat16))
        feed_out = feed_out + term.astype(jnp.float32)
    return feed_out

def one_branch(image_rows, text_rows, length, mod_rows, proj_weight, out_weight, expand_weight, reduce_weight, qk_gain, final_weight):
    h_img = modulate(image_rows, mod_rows[0], mod_rows[1])
    h_txt = modulate(text_rows, mod_rows[4], mod_rows[3])
    img_proj = jnp.stack([jnp.dot(h_img, proj_weight[j], preferred_element_type=jnp.float32) for j in range(3)])
    txt_proj = jnp.stack([jnp.dot(h_txt, proj_weight[j], preferred_element_type=jnp.float32) for j in (3, 4)])
    img_set, txt_set = finish(img_proj, txt_proj, qk_gain)
    key_rows = jnp.concatenate([img_set[1], txt_set[0]], axis=0)
    value_rows = jnp.concatenate([img_set[2], txt_set[1]], axis=0)
    usable = jnp.concatenate([jnp.ones((IMG,), dtype=bool), jnp.arange(TXT, dtype=jnp.int32) < length])
    query_stack = img_set[0].reshape(IMG, HEADS, HD).transpose(1, 0, 2)
    key_stack = key_rows.reshape(IMG + TXT, HEADS, HD).transpose(1, 0, 2)
    value_stack = value_rows.reshape(IMG + TXT, HEADS, HD).transpose(1, 0, 2)

    def per_head(triple):
        return head_attention(triple[0], triple[1], triple[2], usable)
    mixed = lax.map(per_head, (query_stack, key_stack, value_stack))
    mixed = mixed.transpose(1, 0, 2).reshape(IMG, INNER)
    grouped = mixed.reshape(IMG, N_ULYSSES, INNER // N_ULYSSES).astype(jnp.float32)
    weight_groups = out_weight.reshape(N_ULYSSES, INNER // N_ULYSSES, D).astype(jnp.float32)
    group_terms = jnp.einsum('igc,gcd->gid', grouped, weight_groups, precision=lax.Precision.HIGHEST)
    group_terms = lax.optimization_barrier(group_terms.astype(jnp.bfloat16))
    attended = lax.optimization_barrier(jnp.sum(group_terms.astype(jnp.float32), axis=0))
    residual = image_rows.astype(jnp.float32) + mod_rows[2] * attended
    feed_input = modulate(residual, mod_rows[7], mod_rows[8])
    feed_out = feed_forward(feed_input, expand_weight, reduce_weight)
    second_residual = residual + mod_rows[9] * feed_out
    final_rows = modulate(second_residual, mod_rows[6], mod_rows[5])
    noise = jnp.dot(final_rows, final_weight, preferred_element_type=jnp.float32)
    noise = noise.reshape(IMG // IMG_DEV, IMG_DEV, 2, 2, LAT).transpose(4, 0, 2, 1, 3)
    return noise.reshape(LAT, 2 * IMG // IMG_DEV, 2 * IMG_DEV)

def reference(img_tokens, text_tokens, text_lengths, timestep, pooled, time_weight, time_second, mod_weight, proj_weight, out_weight, expand_weight, reduce_weight, qk_gain, final_weight):
    sinusoid_rows = sinusoid(timestep, time_weight.shape[0]).astype(jnp.bfloat16)
    time_hidden = jax.nn.silu(jnp.dot(sinusoid_rows, time_weight, preferred_element_type=jnp.float32)).astype(jnp.bfloat16)
    time_embed = jnp.dot(time_hidden, time_second, preferred_element_type=jnp.float32)
    acted = jax.nn.silu(time_embed[None] + pooled).astype(jnp.bfloat16)
    modulation = jnp.dot(acted.reshape(2 * PROMPTS, D), mod_weight, preferred_element_type=jnp.float32)
    modulation = modulation.reshape(2, PROMPTS, 10, D)
    results = []
    for prompt in range(PROMPTS):
        noises = []
        for branch in range(2):
            noises.append(one_branch(img_tokens[branch, prompt], text_tokens[branch, prompt], text_lengths[branch, prompt], modulation[branch, prompt], proj_weight, out_weight, expand_weight, reduce_weight, qk_gain, final_weight))
        noise_cond = noises[0]
        noise_uncond = noises[1]
        results.append(noise_uncond + GUIDANCE * (noise_cond - noise_uncond))
    return jnp.stack(results)
```

```python
import math

import jax
import jax.numpy as jnp
from jax import lax
from jax.experimental import pallas as pl
from jax.experimental.pallas import tpu as pltpu
from jax.sharding import PartitionSpec as P

GUIDANCE = 3.5
LN_EPS = 1e-06
RMS_EPS = 1e-06
NEG_FILL = -1e30
block_keys = 512


def from_partner(value, axis, stride):
    mask = 2**stride
    pairs = [(source, source ^ mask) for source in range(lax.axis_size(axis))]
    return lax.ppermute(value, axis, pairs)


def sinusoid(timestep, feature_count):
    half_width = feature_count // 2
    frequency = jnp.exp(-math.log(10000.0) * jnp.arange(half_width, dtype=jnp.float32) / half_width)
    angles = timestep.astype(jnp.float32)[:, None] * frequency[None, :]
    return jnp.concatenate([jnp.cos(angles), jnp.sin(angles)], axis=1)


def layer_norm(values):
    average = jnp.mean(values, axis=-1, keepdims=True)
    centred = values - average
    variance = jnp.mean(centred * centred, axis=-1, keepdims=True)
    return centred * lax.rsqrt(variance + LN_EPS)


def modulate(values, shift, scale):
    return (layer_norm(values.astype(jnp.float32)) * (1.0 + scale) + shift).astype(jnp.bfloat16)


def rms_heads(values, gain):
    head_size = gain.shape[0]
    shaped = values.reshape(values.shape[:-1] + (values.shape[-1] // head_size, head_size))
    inverse = lax.rsqrt(jnp.mean(shaped * shaped, axis=-1, keepdims=True) + RMS_EPS)
    return (shaped * inverse * gain).reshape(values.shape).astype(jnp.bfloat16)


def finish(img_proj, txt_proj, gain_rows):
    img_set = jnp.stack(
        [
            rms_heads(img_proj[0], gain_rows[0]),
            rms_heads(img_proj[1], gain_rows[1]),
            img_proj[2].astype(jnp.bfloat16),
        ]
    )
    txt_set = jnp.stack([rms_heads(txt_proj[0], gain_rows[2]), txt_proj[1].astype(jnp.bfloat16)])
    return (img_set, txt_set)


def attend(state_now, query_heads, key_rows, value_rows, usable, scale):
    running_max, running_total, running_sum = state_now
    prompts, query_count, head_count, head_size = query_heads.shape
    key_count = key_rows.shape[1]
    key_heads = key_rows.reshape(prompts, key_count, head_count, head_size)
    value_heads = value_rows.reshape(prompts, key_count, head_count, head_size)
    scores = (
        jnp.einsum("pqhd,pkhd->phqk", query_heads, key_heads, preferred_element_type=jnp.float32)
        * scale
    )
    allowed = usable[:, None, None, :]
    block_max = jnp.max(jnp.where(allowed, scores, NEG_FILL), axis=3)
    new_max = jnp.maximum(running_max, block_max)
    weights = jnp.where(allowed, jnp.exp(scores - new_max[..., None]), 0.0)
    factor = jnp.exp(running_max - new_max)
    running_total = running_total * factor + jnp.sum(weights, axis=3)
    update = jnp.einsum(
        "phqk,pkhd->pqhd",
        weights.astype(jnp.bfloat16),
        value_heads,
        preferred_element_type=jnp.float32,
    )
    running_sum = running_sum * factor.transpose(0, 2, 1)[..., None] + update
    return (new_max, running_total, running_sum)


def attend_rows(state_now, query_heads, key_value, usable, scale):
    key_count = key_value.shape[2]
    for first_key in range(0, key_count, block_keys):
        last_key = min(first_key + block_keys, key_count)
        state_now = attend(
            state_now,
            query_heads,
            key_value[0, :, first_key:last_key],
            key_value[1, :, first_key:last_key],
            usable[:, first_key:last_key],
            scale,
        )
    return state_now


def make_fold(query_heads, lengths, img_span, txt_span, scale):
    span = img_span + txt_span

    def fold(state_now, kv_piece, first_row):
        key_count = kv_piece.shape[2]
        positions = jnp.arange(key_count, dtype=jnp.int32)
        shard_index = positions // span
        offset = positions - shard_index * span
        text_slot = offset - img_span
        usable = (offset < img_span)[None, :] | (text_slot[None, :] < lengths[:, None])
        return attend_rows(state_now, query_heads, kv_piece, usable, scale)

    return fold


def general_body(
    img_tokens,
    text_tokens,
    text_lengths,
    timestep,
    pooled,
    time_weight,
    time_second,
    mod_weight,
    proj_weight,
    out_weight,
    expand_weight,
    reduce_weight,
    qk_gain,
    final_weight,
):
    model_width = img_tokens.shape[3]
    prompts = img_tokens.shape[1]
    head_size = qk_gain.shape[1]
    branch = lax.axis_index("cfg")
    sinusoid_rows = sinusoid(timestep, time_weight.shape[0]).astype(jnp.bfloat16)
    time_hidden = jax.nn.silu(
        jnp.dot(sinusoid_rows, time_weight, preferred_element_type=jnp.float32)
    ).astype(jnp.bfloat16)
    time_part = jnp.dot(time_hidden, time_second, preferred_element_type=jnp.float32)
    time_embed = lax.all_gather(time_part, ("blk", "ulysses", "cfg"), axis=1, tiled=True)
    acted = jax.nn.silu(time_embed[None] + pooled).astype(jnp.bfloat16)
    mod_part = jnp.einsum("bpd,dc->bpc", acted, mod_weight, preferred_element_type=jnp.float32)
    mod_all = lax.all_gather(mod_part, ("blk", "ulysses", "cfg"), axis=2, tiled=True)
    own_mod = lax.dynamic_index_in_dim(mod_all, branch, 0, keepdims=False).reshape(
        prompts, 10, model_width
    )
    image_rows = img_tokens[0]
    text_rows = text_tokens[0]
    lengths = text_lengths[0]
    h_img = modulate(image_rows, own_mod[:, 0:1], own_mod[:, 1:2])
    h_txt = modulate(text_rows, own_mod[:, 4:5], own_mod[:, 3:4])
    rows_img, rows_txt = (
        lax.all_gather(h_img, "ulysses", axis=1, tiled=True),
        lax.all_gather(h_txt, "ulysses", axis=1, tiled=True),
    )
    img_span = rows_img.shape[1]
    txt_span = rows_txt.shape[1]
    img_count = 3 * prompts * img_span
    weight_piece = lax.all_gather(proj_weight, "cfg", axis=2, tiled=True)
    columns = weight_piece.shape[2]
    img_part = jnp.einsum(
        "prd,jdc->jprc", rows_img, weight_piece[0:3], preferred_element_type=jnp.float32
    )
    txt_part = jnp.einsum(
        "prd,jdc->jprc", rows_txt, weight_piece[3:5], preferred_element_type=jnp.float32
    )
    stacked_rows = jnp.concatenate(
        [img_part.reshape(-1, columns), txt_part.reshape(-1, columns)], axis=0
    )
    img_proj = stacked_rows[:img_count].reshape(3, prompts, img_span, -1)
    txt_proj = stacked_rows[img_count:].reshape(2, prompts, txt_span, -1)
    img_set, txt_set = finish(img_proj, txt_proj, qk_gain)
    inner_local = img_set.shape[3]
    head_count = inner_local // head_size
    query_heads = img_set[0].reshape(prompts, img_span, head_count, head_size)
    scale = 1.0 / math.sqrt(head_size)
    start_state = (
        jnp.full((prompts, head_count, img_span), NEG_FILL, jnp.float32),
        jnp.zeros((prompts, head_count, img_span), jnp.float32),
        jnp.zeros((prompts, img_span, head_count, head_size), jnp.float32),
    )
    text_kv = lax.all_gather(jnp.stack([txt_set[0], txt_set[1]]), "blk", axis=2, tiled=True)
    slot_usable = jnp.arange(text_kv.shape[2], dtype=jnp.int32)[None, :] < lengths[:, None]
    text_state = attend_rows(start_state, query_heads, text_kv, slot_usable, scale)
    image_kv = jnp.stack([img_set[1], img_set[2]])
    fold = make_fold(query_heads, lengths, img_span, 0, scale)
    final_state = fold(
        text_state, lax.all_gather(image_kv, "blk", axis=2, tiled=True), jnp.int32(0)
    )
    running_max, running_total, running_sum = final_state
    mixed = (running_sum / running_total.transpose(0, 2, 1)[..., None]).astype(jnp.bfloat16)
    mixed_rows = mixed.reshape(prompts, img_span, inner_local).transpose(1, 0, 2)
    out_gathered = lax.all_gather(out_weight, "cfg", axis=0, tiled=True)
    token_count = image_rows.shape[1]
    segment = mixed_rows
    attended = lax.psum_scatter(
        jnp.einsum("rpc,cd->rpd", segment, out_gathered, preferred_element_type=jnp.float32).astype(
            jnp.bfloat16
        ),
        "ulysses",
        scatter_dimension=0,
        tiled=True,
    ).astype(jnp.float32)
    attended = attended.transpose(1, 0, 2)
    residual = image_rows.astype(jnp.float32) + own_mod[:, 2:3] * attended
    feed_input = modulate(residual, own_mod[:, 7:8], own_mod[:, 8:9]).reshape(
        prompts * token_count, model_width
    )
    feed_all = lax.all_gather(feed_input, ("ulysses", "cfg"), axis=0, tiled=True)
    columns = feed_all
    pre_active = jnp.dot(
        columns,
        lax.all_gather(expand_weight, "blk", axis=0, tiled=True),
        preferred_element_type=jnp.float32,
    )
    feed_hidden = jax.nn.gelu(pre_active, approximate=True).astype(jnp.bfloat16)
    reduce_full = lax.all_gather(reduce_weight, "blk", axis=1, tiled=True)
    segment = feed_hidden
    feed_out = lax.psum_scatter(
        jnp.dot(segment, reduce_full, preferred_element_type=jnp.float32).astype(jnp.bfloat16),
        ("ulysses", "cfg"),
        scatter_dimension=0,
        tiled=True,
    ).astype(jnp.float32)
    second_residual = residual + own_mod[:, 9:10] * feed_out.reshape(
        prompts, token_count, model_width
    )
    final_rows = modulate(second_residual, own_mod[:, 6:7], own_mod[:, 5:6])
    noise = jnp.einsum("prd,dc->prc", final_rows, final_weight, preferred_element_type=jnp.float32)
    latent_channels = final_weight.shape[1] // 4
    noise_own = noise.reshape(prompts, token_count, 2, 2, latent_channels).transpose(0, 4, 2, 1, 3)
    noise_own = noise_own.reshape(prompts, latent_channels, 2, 2 * token_count)
    kept_row = lax.dynamic_slice_in_dim(noise_own, branch, 1, 2)
    sent_row = lax.dynamic_slice_in_dim(noise_own, 1 - branch, 1, 2)
    noise_pair = from_partner(sent_row, "cfg", 0)
    noise_cond = jnp.where(branch == 0, kept_row, noise_pair)
    noise_uncond = jnp.where(branch == 0, noise_pair, kept_row)
    return noise_uncond + GUIDANCE * (noise_cond - noise_uncond)


def swap(value, axis, mask):
    if mask == 0:
        return value
    pairs = [(source, source ^ mask) for source in range(lax.axis_size(axis))]
    return lax.ppermute(value, axis, pairs)


def low_bit(number):
    return number & -number


def gather_relative(value, z_size, x_size):
    along = {0: value}
    order = [bit for bit in (1 << k for k in reversed(range(z_size.bit_length() - 1)))]
    for bit in order:
        along[bit] = swap(value, "blk", bit)
    for b in range(1, z_size):
        if b not in along:
            along[b] = swap(along[b & (b - 1)], "blk", low_bit(b))
    pieces = []
    for b in range(z_size):
        row = {0: along[b]}
        for a in range(1, x_size):
            row[a] = swap(row[a & (a - 1)], "ulysses", low_bit(a))
        pieces.extend(row[a] for a in range(x_size))
    return pieces


def attention_kernel(image_ref, text_ref, gain_ref, allowed_ref, out_ref):
    head_size = gain_ref.shape[1]
    inner = out_ref.shape[1]
    scale = 1.0 / math.sqrt(head_size)
    allowed = allowed_ref[...] > 0

    def normal(values, gain):
        inverse = lax.rsqrt(jnp.mean(values * values, axis=-1, keepdims=True) + RMS_EPS)
        return (values * inverse * gain).astype(jnp.bfloat16)

    def cross(left, right):
        return lax.dot_general(left, right, (((1,), (1,)), ((), ())), preferred_element_type=jnp.float32)

    for head in range(inner // head_size):
        at = head * head_size
        query = normal(image_ref[:, at : at + head_size], gain_ref[0:1, :])
        key = normal(image_ref[:, inner + at : inner + at + head_size], gain_ref[1:2, :])
        value = image_ref[:, 2 * inner + at : 2 * inner + at + head_size].astype(jnp.bfloat16)
        text_key = normal(text_ref[:, at : at + head_size], gain_ref[2:3, :])
        text_value = text_ref[:, inner + at : inner + at + head_size].astype(jnp.bfloat16)
        scores = cross(query, key) * scale
        text_scores = jnp.where(allowed, cross(query, text_key) * scale, NEG_FILL)
        top = jnp.maximum(
            jnp.max(scores, axis=1, keepdims=True), jnp.max(text_scores, axis=1, keepdims=True)
        )
        weights = jnp.exp(scores - top)
        text_weights = jnp.where(allowed, jnp.exp(text_scores - top), 0.0)
        total = jnp.sum(weights, axis=1, keepdims=True) + jnp.sum(text_weights, axis=1, keepdims=True)
        mixed = jnp.dot(
            weights.astype(jnp.bfloat16), value, preferred_element_type=jnp.float32
        ) + jnp.dot(text_weights.astype(jnp.bfloat16), text_value, preferred_element_type=jnp.float32)
        out_ref[:, at : at + head_size] = (mixed / total).astype(jnp.bfloat16)


def attention(image_proj, text_proj, gain, allowed):
    rows = image_proj.shape[0]
    inner = image_proj.shape[1] // 3
    vmem = pl.BlockSpec(memory_space=pltpu.VMEM)
    return pl.pallas_call(
        attention_kernel,
        out_shape=jax.ShapeDtypeStruct((rows, inner), jnp.bfloat16),
        in_specs=[vmem] * 4,
        out_specs=vmem,
        name="attention",
    )(image_proj, text_proj, gain, allowed)


def branch_body(
    img_tokens,
    text_tokens,
    text_lengths,
    timestep,
    pooled,
    time_weight,
    time_second,
    mod_weight,
    proj_weight,
    out_weight,
    expand_weight,
    reduce_weight,
    qk_gain,
    final_weight,
):
    model_width = img_tokens.shape[3]
    y_size = lax.axis_size("groups")
    z_size = lax.axis_size("blk")
    x_size = lax.axis_size("ulysses")
    c_size = lax.axis_size("cfg")
    flat_size = z_size * x_size
    branch = lax.axis_index("cfg")
    z_index = lax.axis_index("blk")
    x_index = lax.axis_index("ulysses")
    y_index = lax.axis_index("groups")
    all_axes = ("blk", "ulysses", "cfg")

    image_rows = img_tokens[0, 0]
    text_rows = text_tokens[0, 0]
    image_count = image_rows.shape[0]
    text_count = text_rows.shape[0]
    pieces = gather_relative(jnp.concatenate([image_rows, text_rows], axis=0), z_size, x_size)

    sinusoid_rows = sinusoid(timestep, time_weight.shape[0]).astype(jnp.bfloat16)
    time_hidden = jax.nn.silu(
        jnp.dot(sinusoid_rows, time_weight, preferred_element_type=jnp.float32)
    ).astype(jnp.bfloat16)
    time_part = jnp.dot(time_hidden, time_second, preferred_element_type=jnp.float32)
    device_count = flat_size * c_size
    time_embed = lax.all_to_all(
        jnp.broadcast_to(time_part, (device_count, time_part.shape[1])), all_axes, 0, 0, tiled=True
    ).reshape(1, model_width)
    acted = jax.nn.silu(time_embed + pooled[:, 0]).astype(jnp.bfloat16)
    mod_part = jnp.dot(acted, mod_weight, preferred_element_type=jnp.float32)
    modulation = lax.all_to_all(jnp.tile(mod_part, (flat_size, 1)), all_axes, 0, 0, tiled=True)
    modulation = modulation.reshape(10, model_width)

    def mod_row(block):
        return modulation[block : block + 1]

    own_columns = proj_weight.shape[2] // z_size
    own_proj = lax.dynamic_slice_in_dim(proj_weight, z_index * own_columns, own_columns, 2)
    pair_proj = swap(own_proj, "cfg", 1)
    both = (own_proj, pair_proj)
    image_weight = jnp.concatenate([half[j] for j in range(3) for half in both], axis=1)
    text_weight = jnp.concatenate([half[j] for j in range(3, 5) for half in both], axis=1)

    out_rows = out_weight.shape[0] // z_size
    own_out = jnp.concatenate(
        [
            lax.dynamic_slice_in_dim(out_weight, (z_index ^ b) * out_rows, out_rows, 0)
            for b in range(z_size)
        ],
        axis=0,
    )
    out_sets = []
    for a in range(x_size):
        if a == 0:
            mine = own_out
        elif y_size == 2:
            half_rows = own_out.shape[0] // 2
            part = swap(
                lax.dynamic_slice_in_dim(own_out, y_index * half_rows, half_rows, 0), "ulysses", a
            )
            other = swap(part, "groups", 1)
            mine = jnp.zeros_like(own_out)
            mine = lax.dynamic_update_slice_in_dim(mine, part, y_index * half_rows, 0)
            mine = lax.dynamic_update_slice_in_dim(mine, other, (1 - y_index) * half_rows, 0)
        else:
            mine = swap(own_out, "ulysses", a)
        out_sets.append((mine, swap(mine, "cfg", 1)))

    d_rows = expand_weight.shape[0]
    units = expand_weight.shape[1] // z_size
    shares = y_size if y_size == 2 else 1
    expand_half = d_rows // shares
    reduce_half = units // shares
    expand_own = jnp.zeros((z_size, d_rows, units), jnp.bfloat16)
    reduce_own = jnp.zeros((z_size, units, d_rows), jnp.bfloat16)
    expand_first = lax.dynamic_slice_in_dim(expand_weight, z_index * units, units, 1)
    reduce_first = lax.dynamic_slice_in_dim(reduce_weight, z_index * units, units, 0)
    expand_own = lax.dynamic_update_slice(expand_own, expand_first[None], (z_index, 0, 0))
    reduce_own = lax.dynamic_update_slice(reduce_own, reduce_first[None], (z_index, 0, 0))
    share = y_index if shares == 2 else 0
    expand_parts = []
    reduce_parts = []
    for b in range(1, z_size):
        piece = lax.dynamic_slice(
            expand_weight, (share * expand_half, (z_index ^ b) * units), (expand_half, units)
        )
        expand_parts.append(swap(piece, "blk", b))
    for b in range(1, z_size):
        piece = lax.dynamic_slice_in_dim(
            reduce_weight, (z_index ^ b) * units + share * reduce_half, reduce_half, 0
        )
        reduce_parts.append(swap(piece, "blk", b))

    def place(whole, parts, half):
        for b in range(1, z_size):
            whole = lax.dynamic_update_slice(
                whole, parts[b - 1][None], (z_index ^ b, share * half, 0)
            )
        if shares == 2:
            others = swap(jnp.stack(parts), "groups", 1)
            for b in range(1, z_size):
                whole = lax.dynamic_update_slice(
                    whole, others[b - 1][None], (z_index ^ b, (1 - share) * half, 0)
                )
        return whole

    expand_own = place(expand_own, expand_parts, expand_half)
    reduce_own = place(reduce_own, reduce_parts, reduce_half)
    expand_sets = [expand_own, swap(expand_own, "cfg", 1)]
    reduce_sets = [reduce_own, swap(reduce_own, "cfg", 1)]

    image_all = jnp.concatenate([piece[:image_count] for piece in pieces], axis=0)
    text_all = jnp.concatenate([piece[image_count:] for piece in pieces], axis=0)
    h_img = modulate(image_all, mod_row(0), mod_row(1))
    h_txt = modulate(text_all, mod_row(4), mod_row(3))
    image_proj = jnp.dot(h_img, image_weight, preferred_element_type=jnp.float32)
    text_proj = jnp.dot(h_txt, text_weight, preferred_element_type=jnp.float32)
    slots = jnp.concatenate(
        [
            ((z_index ^ b) * x_size + (x_index ^ a)) * text_count + jnp.arange(text_count, dtype=jnp.int32)
            for b in range(z_size)
            for a in range(x_size)
        ]
    )
    allowed = (slots < text_lengths[0, 0]).astype(jnp.int32)[None, :]
    mixed = attention(image_proj, text_proj, qk_gain, allowed)

    mixed_pieces = gather_relative(mixed, z_size, x_size)
    head_columns = mixed.shape[1] // 2
    attended = None
    for a in range(x_size):
        ordered = []
        for b in range(z_size):
            piece = mixed_pieces[b * x_size + a].reshape(flat_size, image_count, -1)
            shift = b * x_size + a
            ordered.append(
                jnp.concatenate([piece[r ^ shift] for r in range(flat_size)], axis=0)
            )
        columns = jnp.concatenate(
            [
                piece[:, half * head_columns : (half + 1) * head_columns]
                for half in range(2)
                for piece in ordered
            ],
            axis=1,
        )
        weight = jnp.concatenate(out_sets[a], axis=0)
        term = jnp.dot(columns, weight, preferred_element_type=jnp.float32).astype(jnp.bfloat16)
        term = term.astype(jnp.float32)
        attended = term if attended is None else attended + term
    residual = image_all.astype(jnp.float32) + mod_row(2) * attended
    feed_input = modulate(residual, mod_row(7), mod_row(8))
    residual_own = residual[:image_count]

    hidden = [
        jax.nn.gelu(
            jnp.dot(
                feed_input, part.reshape(model_width, units), preferred_element_type=jnp.float32
            ),
            approximate=True,
        ).astype(jnp.bfloat16)
        for part in expand_sets
    ]
    partial = []
    for block in range(z_size):
        total = jnp.dot(hidden[0], reduce_sets[0][block], preferred_element_type=jnp.float32)
        total = total + jnp.dot(hidden[1], reduce_sets[1][block], preferred_element_type=jnp.float32)
        partial.append(total.astype(jnp.bfloat16))

    def halve(values, axis, bit):
        mask = bit * x_size if axis == "blk" else bit
        kept = [r for r in values if not r & mask]
        sent = jnp.concatenate([values[r | mask] for r in kept], axis=0)
        got = swap(sent.astype(jnp.bfloat16), axis, bit)
        rows = image_count
        return {
            r: values[r].astype(jnp.float32) + got[i * rows : (i + 1) * rows].astype(jnp.float32)
            for i, r in enumerate(kept)
        }

    z_steps = [("blk", 1 << k) for k in range(z_size.bit_length() - 1)]
    x_steps = [("ulysses", 1 << k) for k in range(x_size.bit_length() - 1)]
    first_order = x_steps + z_steps
    second_order = z_steps[:1] + x_steps + z_steps[1:]
    blocks_half = z_size // 2
    feed_parts = []
    for blocks, order in ((partial[:blocks_half], first_order), (partial[blocks_half:], second_order)):
        wide = jnp.concatenate(blocks, axis=1)
        values = {r: wide[r * image_count : (r + 1) * image_count] for r in range(flat_size)}
        for axis, bit in order:
            values = halve(values, axis, bit)
        feed_parts.append(values[0])
    feed_out = jnp.concatenate(feed_parts, axis=1)

    second_residual = residual_own + mod_row(9) * feed_out
    final_rows = modulate(second_residual, mod_row(6), mod_row(5))
    noise = jnp.dot(final_rows, final_weight, preferred_element_type=jnp.float32)
    latent_channels = final_weight.shape[1] // 4
    noise_own = noise.reshape(1, image_count, 2, 2, latent_channels).transpose(0, 4, 2, 1, 3)
    noise_own = noise_own.reshape(1, latent_channels, 2, 2 * image_count)
    kept_row = lax.dynamic_slice_in_dim(noise_own, branch, 1, 2)
    sent_row = lax.dynamic_slice_in_dim(noise_own, 1 - branch, 1, 2)
    noise_pair = from_partner(sent_row, "cfg", 0)
    noise_cond = jnp.where(branch == 0, kept_row, noise_pair)
    noise_uncond = jnp.where(branch == 0, noise_pair, kept_row)
    return noise_uncond + GUIDANCE * (noise_cond - noise_uncond)


def power_of_two(number):
    return number > 0 and number & (number - 1) == 0


def body(*arrays):
    img_tokens, proj_weight, expand_weight, qk_gain = arrays[0], arrays[8], arrays[10], arrays[12]
    z_size = lax.axis_size("blk")
    x_size = lax.axis_size("ulysses")
    by_branch = (
        img_tokens.shape[1] == 1
        and z_size > 1
        and power_of_two(z_size)
        and power_of_two(x_size)
        and proj_weight.shape[2] % (z_size * qk_gain.shape[1]) == 0
        and expand_weight.shape[1] % (32 * z_size) == 0
        and expand_weight.shape[0] % 32 == 0
    )
    return branch_body(*arrays) if by_branch else general_body(*arrays)


def solution(mesh):
    in_specs = (
        P("cfg", "groups", ("blk", "ulysses"), None),
        P("cfg", "groups", ("blk", "ulysses"), None),
        P("cfg", "groups"),
        P("groups"),
        P(None, "groups", None),
        P(),
        P(None, ("blk", "ulysses", "cfg")),
        P(None, ("blk", "ulysses", "cfg")),
        P(None, None, ("ulysses", "cfg")),
        P(("ulysses", "cfg"), None),
        P("blk", ("ulysses", "cfg")),
        P(("ulysses", "cfg"), "blk"),
        P(),
        P(),
    )
    out_specs = P("groups", None, ("blk", "ulysses", "cfg"), None)
    return jax.shard_map(body, mesh=mesh, in_specs=in_specs, out_specs=out_specs, check_vma=False)
```
